32 devices in a mesh: seq: 8 (over y, x, core), head: 4 (over z).
Axes of the slice: x: 2, y: 2, z: 4, core: 2. Of those that a mesh axis runs over, the one named last changes fastest.
Arguments:
- probe_vectors: bfloat16 [2048, 4096], P('seq', 'head'), may hold values from -6 to 6
- source_vectors: bfloat16 [2048, 4096], P('seq', 'head'), may hold values from -6 to 6
- content_vectors: bfloat16 [2048, 4096], P('seq', 'head'), may hold values from -6 to 6
- probe_direction_matrix: bfloat16 [2048, 4096], P('seq', 'head'), may hold values from -6 to 6
- probe_direction_source: bfloat16 [2048, 4096], P('seq', 'head'), may hold values from -6 to 6
- content_direction: bfloat16 [2048, 4096], P('seq', 'head'), may hold values from -6 to 6
- head_table_indices: int32 [32], P('head'), may hold values from 0 to 7
- reset_flags: int32 [2048], P('seq'), may hold values 0 or 1
- projection_matrix: bfloat16 [4096, 4096], P('head'), may hold values from -0.09375 to 0.09375
- regression_goal: bfloat16 [2048, 4096], P('seq'), may hold values from -6 to 6
Outputs:
- hess_q: bfloat16 [2048, 4096], P('seq', 'head')
- hess_k: bfloat16 [2048, 4096], P('seq', 'head')
- hess_v: bfloat16 [2048, 4096], P('seq', 'head')
The draws below stay inside these ranges and needn't reach their ends.
All inputs are finite; a program needn't handle non-finite values. No bound on the sum of `reset_flags` on one device may be relied on, other than what follows from the above.
Results may differ from the reference program's by a relative error of at most 0.024.
Values may be sent and summed in bfloat16 or wider, within the bound.
A program may use at most 128 MiB of HBM per device.

```python
import math
import jax
import jax.numpy as jnp
from jax import lax

D = 4096
HEADS = 32
HEAD_DIM = 128
SPAN_LENGTH = 256
LEVELS = 8
SEQUENCE_LENGTH = 2048
N_SEQ = 8
N_HEAD = 4


def set_ends(drawn, own_key, smallest, top_value):
    index_at = [jax.random.randint(jax.random.fold_in(own_key, axis), (), 0, length) for axis, length in enumerate(drawn.shape)]
    main_axis = drawn.shape.index(max(drawn.shape))
    neighbour = index_at[:main_axis] + [(index_at[main_axis] + 1) % drawn.shape[main_axis]] + index_at[main_axis + 1:]
    return drawn.at[tuple(index_at)].set(smallest).at[tuple(neighbour)].set(top_value)


def levels(own_key, extent, pieces, least, top_value):
    factor_of = 1.0
    for axis_at, blocks in pieces:
        draws = jax.random.uniform(jax.random.fold_in(jax.random.fold_in(own_key, 6), axis_at), (blocks,), jnp.float32, least / len(pieces), top_value / len(pieces))
        factor_of = factor_of * jnp.repeat(jnp.exp(draws), extent[axis_at] // blocks).reshape((-1,) + (1,) * (len(extent) - 1 - axis_at))
    return factor_of


def noise(stream_key, shape, width, most, shards=(), held_as=jnp.bfloat16):
    entries = width * jax.random.normal(stream_key, shape, jnp.float32)
    if shards:
        entries = entries * levels(stream_key, shape, shards, -0.22, 0.18)
    return jnp.clip(entries, -most, most).astype(held_as)


def setup_inputs(seed: int = 0) -> dict:
    streams_of = jax.random.split(jax.random.key(seed), 11)
    probe_vectors = noise(streams_of[0], (SEQUENCE_LENGTH, HEADS * HEAD_DIM), 1.0, 6.0, ((0, 8), (1, 4)))
    source_vectors = noise(streams_of[1], (SEQUENCE_LENGTH, HEADS * HEAD_DIM), 1.0, 6.0, ((0, 8), (1, 4)))
    content_vectors = noise(streams_of[2], (SEQUENCE_LENGTH, HEADS * HEAD_DIM), 1.0, 6.0, ((0, 8), (1, 4)))
    probe_direction_matrix = noise(streams_of[3], (SEQUENCE_LENGTH, HEADS * HEAD_DIM), 1.0, 6.0, ((0, 8), (1, 4)))
    probe_direction_source = noise(streams_of[4], (SEQUENCE_LENGTH, HEADS * HEAD_DIM), 1.0, 6.0, ((0, 8), (1, 4)))
    content_direction = noise(streams_of[5], (SEQUENCE_LENGTH, HEADS * HEAD_DIM), 1.0, 6.0, ((0, 8), (1, 4)))
    head_table_indices = set_ends(jax.random.randint(streams_of[6], (HEADS,), 0, LEVELS), jax.random.fold_in(streams_of[6], 1), 0, LEVELS - 1).astype(jnp.int32)
    reset_flags = set_ends((jax.random.randint(streams_of[7], (SEQUENCE_LENGTH,), 0, SEQUENCE_LENGTH) < 4).astype(jnp.int32), jax.random.fold_in(streams_of[7], 1), 0, 1)
    projection_matrix = noise(streams_of[8], (HEADS * HEAD_DIM, D), (HEADS * HEAD_DIM) ** -0.5, 0.09375, ((0, 4),))
    regression_goal = noise(streams_of[9], (SEQUENCE_LENGTH, D), 1.0, 6.0, ((0, 8),))
    return {"probe_vectors": probe_vectors, "source_vectors": source_vectors, "content_vectors": content_vectors, "probe_direction_matrix": probe_direction_matrix, "probe_direction_source": probe_direction_source, "content_direction": content_direction, "head_table_indices": head_table_indices, "reset_flags": reset_flags, "projection_matrix": projection_matrix, "regression_goal": regression_goal}


RESET_KEPT_SHARE = 0.7
EPS = 1e-06
HIGHEST = lax.Precision.HIGHEST

def log_gammas(head_table_indices, chain_len):
    fraction = head_table_indices.astype(jnp.float32) / (LEVELS - 1)
    rates = jnp.exp(math.log(1.0 / 32.0) + fraction * math.log(16.0 / chain_len))
    return jnp.log1p(-rates)

def segment_rate_exponents(reset_flags, forgetting_exponent):
    running_number = jnp.cumsum(reset_flags).astype(jnp.float32)
    position_indices = jnp.arange(1, reset_flags.shape[0] + 1).astype(jnp.float32)
    return position_indices[:, None] * forgetting_exponent[None, :] + math.log(RESET_KEPT_SHARE) * running_number[:, None]

def block_out(q, k, v, state, fading_rate_exponent):
    length = q.shape[0]
    scale = q.shape[2] ** (-0.5)
    scores = jnp.einsum('thd,shd->hts', q, k * scale, precision=HIGHEST)
    later = lax.broadcasted_iota(jnp.int32, (length, length), 0) >= lax.broadcasted_iota(jnp.int32, (length, length), 1)
    trans = fading_rate_exponent.T
    spread = trans[:, :, None] - trans[:, None, :]
    weights = jnp.where(later[None], jnp.exp(jnp.where(later[None], spread, 0.0)), 0.0)
    inner = jnp.einsum('hts,she->the', scores * weights, v, precision=HIGHEST)
    outer = jnp.exp(fading_rate_exponent)[:, :, None] * jnp.einsum('thd,hde->the', q, state, precision=HIGHEST)
    return inner + outer

def block_state(k, v, fading_rate_exponent):
    scale = k.shape[2] ** (-0.5)
    weights = jnp.exp(fading_rate_exponent[-1][None, :] - fading_rate_exponent)
    return jnp.einsum('shd,she->hde', k * (scale * weights[:, :, None]), v, precision=HIGHEST)

def group_norm(outputs):
    return outputs * lax.rsqrt(lax.optimization_barrier(jnp.mean(outputs * outputs, axis=-1, keepdims=True)) + EPS)

def head_sum(rows, weight):
    columns = rows.shape[1] // N_HEAD
    total_sum = jnp.zeros((rows.shape[0], weight.shape[1]), jnp.float32)
    for group in range(N_HEAD):
        piece = jnp.dot(rows[:, group * columns:(group + 1) * columns], weight[group * columns:(group + 1) * columns], preferred_element_type=jnp.float32)
        piece = lax.optimization_barrier(piece.astype(jnp.bfloat16)).astype(jnp.float32)
        total_sum = total_sum + piece
    return total_sum

def reference(probe_vectors, source_vectors, content_vectors, probe_direction_matrix, probe_direction_source, content_direction, head_table_indices, reset_flags, projection_matrix, regression_goal):

    def blocks(array):
        return array.astype(jnp.float32).reshape(N_SEQ, SPAN_LENGTH, HEADS, HEAD_DIM)
    q_rows, k_rows, v_rows = (blocks(probe_vectors), blocks(source_vectors), blocks(content_vectors))
    q_tan, k_tan, v_tan = (blocks(probe_direction_matrix), blocks(probe_direction_source), blocks(content_direction))
    forgetting_exponent = log_gammas(head_table_indices, float(SEQUENCE_LENGTH))
    fading_rate_exponent = jax.vmap(segment_rate_exponents, (0, None))(reset_flags.reshape(N_SEQ, SPAN_LENGTH), forgetting_exponent)
    decay_all = jnp.exp(fading_rate_exponent[:, -1, :])

    def own_state(item):
        key_b, value_b, key_t, value_t, logs_b = item
        return jax.jvp(lambda a, b: block_state(a, b, logs_b), (key_b, value_b), (key_t, value_t))
    state_own, state_tan = lax.map(own_state, (k_rows, v_rows, k_tan, v_tan, fading_rate_exponent))
    zero_state = jnp.zeros((HEADS, HEAD_DIM, HEAD_DIM), jnp.float32)

    def forward_step(carry, item):
        held, held_tan = carry
        decay_b, own_b, own_t = item
        factor = decay_b[:, None, None]
        return ((held * factor + own_b, held_tan * factor + own_t), (held, held_tan))
    unused_carry, (state_in, state_in_tan) = lax.scan(forward_step, (zero_state, zero_state), (decay_all, state_own, state_tan))
    target_blocks = regression_goal.reshape(N_SEQ, SPAN_LENGTH, D)

    def middle(item):
        q, k, v, qt, kt, vt, state, state_t, logs_b, wanted = item
        outputs, outputs_tan = jax.jvp(lambda a, b, c, d: block_out(a, b, c, d, logs_b), (q, k, v, state), (qt, kt, vt, state_t))
        normed, normed_tan = jax.jvp(group_norm, (outputs,), (outputs_tan,))
        summed = head_sum(normed.reshape(SPAN_LENGTH, -1).astype(jnp.bfloat16), projection_matrix)
        summed_tan = head_sum(normed_tan.reshape(SPAN_LENGTH, -1).astype(jnp.bfloat16), projection_matrix)
        residual = (summed - wanted.astype(jnp.float32)).astype(jnp.bfloat16)
        residual_tan = summed_tan.astype(jnp.bfloat16)
        dims = (((1,), (1,)), ((), ()))
        grad_norm = lax.dot_general(residual, projection_matrix, dims, preferred_element_type=jnp.float32).reshape(SPAN_LENGTH, HEADS, HEAD_DIM)
        grad_norm_tan = lax.dot_general(residual_tan, projection_matrix, dims, preferred_element_type=jnp.float32).reshape(SPAN_LENGTH, HEADS, HEAD_DIM)

        def norm_back(point, cotan):
            return jax.vjp(group_norm, point)[1](cotan)[0]
        grad_out, grad_out_tan = jax.jvp(norm_back, (outputs, grad_norm), (outputs_tan, grad_norm_tan))

        def out_grads(a, b, c, d, g):
            return jax.vjp(lambda a2, b2, c2, d2: block_out(a2, b2, c2, d2, logs_b), a, b, c, d)[1](g)
        primal_g, tangent_g = jax.jvp(out_grads, (q, k, v, state, grad_out), (qt, kt, vt, state_t, grad_out_tan))
        return (tangent_g[0], tangent_g[1], tangent_g[2], primal_g[3], tangent_g[3])
    hess_qb, hess_k1, hess_v1, grad_state, grad_state_tan = lax.map(middle, (q_rows, k_rows, v_rows, q_tan, k_tan, v_tan, state_in, state_in_tan, fading_rate_exponent, target_blocks))

    def reverse_step(carry, item):
        held, held_tan = carry
        decay_b, grad_b, grad_t = item
        factor = decay_b[:, None, None]
        return ((grad_b + factor * held, grad_t + factor * held_tan), (held, held_tan))
    unused_back, (state_cot, state_cot_tan) = lax.scan(reverse_step, (zero_state, zero_state), (decay_all, grad_state, grad_state_tan), reverse=True)

    def last_part(item):
        k, v, kt, vt, cot, cot_t, logs_b = item

        def state_grads(b, c, g):
            return jax.vjp(lambda b2, c2: block_state(b2, c2, logs_b), b, c)[1](g)
        return jax.jvp(state_grads, (k, v, cot), (kt, vt, cot_t))[1]
    hess_k2, hess_v2 = lax.map(last_part, (k_rows, v_rows, k_tan, v_tan, state_cot, state_cot_tan, fading_rate_exponent))
    shape_out = (SEQUENCE_LENGTH, HEADS * HEAD_DIM)
    hess_q = hess_qb.reshape(shape_out).astype(jnp.bfloat16)
    hess_k = (hess_k1 + hess_k2).reshape(shape_out).astype(jnp.bfloat16)
    hess_v = (hess_v1 + hess_v2).reshape(shape_out).astype(jnp.bfloat16)
    return (hess_q, hess_k, hess_v)
```

```python
import math

import jax
import jax.numpy as jnp
from jax import lax
from jax.experimental import pallas as pl
from jax.experimental.pallas import tpu as pltpu
from jax.sharding import PartitionSpec as P

LEVELS = 8


RESET_KEPT_SHARE = 0.7
EPS = 1e-06
HIGHEST = lax.Precision.HIGHEST
PLAIN = lax.Precision.DEFAULT


WAVES = 4
MESH = pl.DeviceIdType.MESH


def scan_kernel(n, flip, state_ref, decay_ref, out_ref, total, msg, got, span, dmsg, dgot, sems):
    me = lax.axis_index("seq")
    core = lax.rem(me, 2)
    mate = me + 1 - 2 * core
    steps = n.bit_length() - 1
    bit_of = [lax.rem(me // (1 << b), 2) for b in range(steps)]
    partner_of = [me + (1 << b) - 2 * (1 << b) * bit_of[b] for b in range(steps)]

    barrier = pltpu.get_barrier_semaphore()
    for b in range(steps):
        pl.semaphore_signal(
            barrier, inc=1, device_id={"seq": partner_of[b]}, device_id_type=MESH
        )
    pl.semaphore_wait(barrier, steps)

    def send(kind, b, src, dst, target):
        copy = pltpu.make_async_remote_copy(
            src_ref=src,
            dst_ref=dst,
            send_sem=sems.at[0, kind, b],
            recv_sem=sems.at[1, kind, b],
            device_id={"seq": target},
            device_id_type=MESH,
        )
        copy.start()
        return copy

    heads = decay_ref.shape[0]
    total[...] = state_ref[...]
    out_ref[...] = jnp.zeros_like(out_ref)
    span[...] = jnp.ones_like(span)
    dmsg[0] = decay_ref[...]
    sent = []
    for b in range(steps):
        msg[b] = total[...].astype(jnp.bfloat16)
        c_decay = send(0, b, dmsg.at[b], dgot.at[b], partner_of[b])
        if b == 0:
            c_state = send(1, b, msg.at[b], got.at[b], partner_of[b])
            c_decay.wait()
            c_state.wait()
        else:
            c_state = send(1, b, msg.at[b, core], got.at[b, core], partner_of[b])
            c_decay.wait()
            c_state.wait()
            c_share = send(2, b, got.at[b, core], got.at[b, core], mate)
            c_share.wait()
        up = bit_of[b] if not flip else 1 - bit_of[b]
        up = up.astype(jnp.float32)
        other = dgot[b]
        own = dmsg[b]
        keep_factor = up + (1.0 - up) * other
        take_factor = up * own + (1.0 - up)
        in_factor = up * span[...]
        for h in range(heads):
            for part in range(2):
                arrived = got[b, part, h].astype(jnp.float32)
                out_ref[part, h] = out_ref[part, h] + arrived * in_factor[h, :1]
                if b < steps - 1:
                    total[part, h] = total[part, h] * keep_factor[h, :1] + arrived * take_factor[h, :1]
        span[...] = span[...] * (up * other + (1.0 - up))
        if b < steps - 1:
            dmsg[b + 1] = own * other


def entering(state, decay, flip, ident):
    n = lax.axis_size("seq")
    steps = n.bit_length() - 1
    heads = decay.shape[0]
    wide = jnp.broadcast_to(decay[:, None, None], (heads, 8, 128))
    return pl.pallas_call(
        lambda *refs: scan_kernel(n, flip, *refs),
        out_shape=jax.ShapeDtypeStruct(state.shape, jnp.float32),
        in_specs=[pl.BlockSpec(memory_space=pltpu.VMEM)] * 2,
        out_specs=pl.BlockSpec(memory_space=pltpu.VMEM),
        scratch_shapes=[
            pltpu.VMEM(state.shape, jnp.float32),
            pltpu.VMEM((steps,) + state.shape, jnp.bfloat16),
            pltpu.VMEM((steps,) + state.shape, jnp.bfloat16),
            pltpu.VMEM(wide.shape, jnp.float32),
            pltpu.VMEM((steps,) + wide.shape, jnp.float32),
            pltpu.VMEM((steps,) + wide.shape, jnp.float32),
            pltpu.SemaphoreType.DMA((2, 3, steps)),
        ],
        compiler_params=pltpu.CompilerParams(collective_id=ident, has_side_effects=True),
    )(state, wide)


def middle_kernel(
    n, z_ref, p_ref, goal_ref, grad_ref, send_up, send_dn, got_up, got_dn, final, ag_up, ag_dn, sems
):
    d = lax.axis_index("head")
    length = goal_ref.shape[0]
    waves, sub = final.shape[0], final.shape[2]

    barrier = pltpu.get_barrier_semaphore()

    def greet(step):
        pl.semaphore_signal(barrier, inc=1, device_id={"head": d + step}, device_id_type=MESH)

    @pl.when(d > 0)
    def _():
        greet(-1)

    @pl.when(d < n - 1)
    def _():
        greet(1)

    pl.semaphore_wait(barrier, jnp.minimum(d, 1) + jnp.minimum(n - 1 - d, 1))

    grad_ref[...] = jnp.zeros_like(grad_ref)

    def copy_of(kind, slot, w, src, dst, step):
        return pltpu.make_async_remote_copy(
            src_ref=src,
            dst_ref=dst,
            send_sem=sems.at[0, kind, slot, w],
            recv_sem=sems.at[1, kind, slot, w],
            device_id={"head": lax.rem(d + step + n, n)},
            device_id_type=MESH,
        )

    def rs_up(r, w):
        return copy_of(0, r - 1, w, send_up.at[r - 1, w], got_up.at[r - 1, w], 1)

    def rs_dn(r, w):
        return copy_of(1, r - 1, w, send_dn.at[r - 1, w], got_dn.at[r - 1, w], -1)

    def gather_up(r, w):
        src = final.at[w] if r == 0 else ag_up.at[r - 1, w]
        return copy_of(2, r, w, src, ag_up.at[r, w], 1)

    def gather_dn(r, w):
        src = final.at[w] if r == 0 else ag_dn.at[r - 1, w]
        return copy_of(3, r, w, src, ag_dn.at[r, w], -1)

    def columns(j, w):
        return pl.ds(pl.multiple_of((j * waves + w) * sub, sub), sub)

    def part_sum(j, w):
        out = jnp.dot(z_ref[...], p_ref[:, columns(j, w)], preferred_element_type=jnp.float32)
        return out.astype(jnp.bfloat16).astype(jnp.float32)

    def back(block, j, w):
        grad_ref[...] += lax.dot_general(
            block,
            p_ref[:, columns(j, w)],
            (((1,), (1,)), ((), ())),
            preferred_element_type=jnp.float32,
        )

    def reduce_phase(r, w):
        @pl.when(d + r < n)
        def _():
            send_up[r - 1, w] = part_sum(d + r, w).astype(jnp.bfloat16)
            if r + 1 < n:

                @pl.when(d > 0)
                def _():
                    rs_up(r + 1, w).wait_recv()
                    send_up[r - 1, w] = (
                        send_up[r - 1, w].astype(jnp.float32)
                        + got_up[r, w].astype(jnp.float32)
                    ).astype(jnp.bfloat16)

            rs_up(r, w).start()

        @pl.when(d - r >= 0)
        def _():
            send_dn[r - 1, w] = part_sum(d - r, w).astype(jnp.bfloat16)
            if r + 1 < n:

                @pl.when(d < n - 1)
                def _():
                    rs_dn(r + 1, w).wait_recv()
                    send_dn[r - 1, w] = (
                        send_dn[r - 1, w].astype(jnp.float32)
                        + got_dn[r, w].astype(jnp.float32)
                    ).astype(jnp.bfloat16)

            rs_dn(r, w).start()

    def final_phase(w, own_ref):
        own_ref[...] = part_sum(d, w)

        @pl.when(d > 0)
        def _():
            rs_up(1, w).wait_recv()
            own_ref[...] += got_up[0, w].astype(jnp.float32)

        @pl.when(d < n - 1)
        def _():
            rs_dn(1, w).wait_recv()
            own_ref[...] += got_dn[0, w].astype(jnp.float32)

        final[w, :length] = (
            own_ref[:length] - goal_ref[:, columns(d, w)].astype(jnp.float32)
        ).astype(jnp.bfloat16)
        final[w, length:] = own_ref[length:].astype(jnp.bfloat16)

        @pl.when(d < n - 1)
        def _():
            gather_up(0, w).start()

        @pl.when(d > 0)
        def _():
            gather_dn(0, w).start()

        back(final[w], d, w)

    def gather_phase(r, w):
        @pl.when(d - r >= 0)
        def _():
            gather_up(r - 1, w).wait_recv()
            if r < n - 1:

                @pl.when(d < n - 1)
                def _():
                    gather_up(r, w).start()

        @pl.when(d + r < n)
        def _():
            gather_dn(r - 1, w).wait_recv()
            if r < n - 1:

                @pl.when(d > 0)
                def _():
                    gather_dn(r, w).start()

        @pl.when(d - r >= 0)
        def _():
            back(ag_up[r - 1, w], d - r, w)

        @pl.when(d + r < n)
        def _():
            back(ag_dn[r - 1, w], d + r, w)

    def run(own_ref):
        phases = 2 * n - 1
        for t in range(phases + waves - 1):
            for w in range(waves):
                p = t - w
                if p < 0 or p >= phases:
                    continue
                if p < n - 1:
                    reduce_phase(n - 1 - p, w)
                elif p == n - 1:
                    final_phase(w, own_ref)
                else:
                    gather_phase(p - n + 1, w)

    pl.run_scoped(run, pltpu.VMEM(final.shape[1:], jnp.float32))

    for w in range(waves):
        for r in range(1, n):

            @pl.when(d + r < n)
            def _():
                rs_up(r, w).wait_send()

            @pl.when(d - r >= 0)
            def _():
                rs_dn(r, w).wait_send()

        for r in range(n - 1):

            @pl.when(jnp.logical_and(d - r >= 0, d < n - 1))
            def _():
                gather_up(r, w).wait_send()

            @pl.when(jnp.logical_and(d + r < n, d > 0))
            def _():
                gather_dn(r, w).wait_send()


def middle(z_rows, projection, goal):
    n = lax.axis_size("head")
    rows, width = z_rows.shape[0], projection.shape[1]
    sub = width // n // WAVES
    lane = (n - 1, WAVES, rows, sub)
    return pl.pallas_call(
        lambda *refs: middle_kernel(n, *refs),
        out_shape=jax.ShapeDtypeStruct((rows, projection.shape[0]), jnp.float32),
        in_specs=[pl.BlockSpec(memory_space=pltpu.VMEM)] * 3,
        out_specs=pl.BlockSpec(memory_space=pltpu.VMEM),
        scratch_shapes=[pltpu.VMEM(lane, jnp.bfloat16)] * 4
        + [pltpu.VMEM(lane[1:], jnp.bfloat16)]
        + [pltpu.VMEM(lane, jnp.bfloat16)] * 2
        + [pltpu.SemaphoreType.DMA((2, 4, n - 1, WAVES))],
        compiler_params=pltpu.CompilerParams(
            collective_id=2, has_side_effects=True, vmem_limit_bytes=60 * 1024 * 1024
        ),
    )(z_rows, projection, goal)


def log_gammas(head_table_indices, chain_len):
    fraction = head_table_indices.astype(jnp.float32) / (LEVELS - 1)
    rates = jnp.exp(math.log(1.0 / 32.0) + fraction * math.log(16.0 / chain_len))
    return jnp.log1p(-rates)


def segment_rate_exponents(reset_flags, forgetting_exponent):
    running_number = jnp.cumsum(reset_flags).astype(jnp.float32)
    position_indices = jnp.arange(1, reset_flags.shape[0] + 1).astype(jnp.float32)
    return (
        position_indices[:, None] * forgetting_exponent[None, :]
        + math.log(RESET_KEPT_SHARE) * running_number[:, None]
    )


def block_out(q, k, v, state, fading_rate_exponent, score_prec):
    length = q.shape[0]
    scale = q.shape[2] ** (-0.5)
    scores = jnp.einsum("thd,shd->hts", q, k, precision=score_prec) * scale
    later = lax.broadcasted_iota(jnp.int32, (length, length), 0) >= lax.broadcasted_iota(
        jnp.int32, (length, length), 1
    )
    trans = fading_rate_exponent.T
    spread = trans[:, :, None] - trans[:, None, :]
    weights = jnp.where(later[None], jnp.exp(jnp.where(later[None], spread, 0.0)), 0.0)
    inner = jnp.einsum("hts,she->the", scores * weights, v, precision=HIGHEST)
    outer = jnp.exp(fading_rate_exponent)[:, :, None] * jnp.einsum(
        "thd,hde->the", q, state, precision=HIGHEST
    )
    return inner + outer


def block_state(k, v, fading_rate_exponent):
    scale = k.shape[2] ** (-0.5)
    weights = jnp.exp(fading_rate_exponent[-1][None, :] - fading_rate_exponent)
    return jnp.einsum("shd,she->hde", k * (scale * weights[:, :, None]), v, precision=HIGHEST)


def group_norm(outputs):
    return outputs * lax.rsqrt(jnp.mean(outputs * outputs, axis=-1, keepdims=True) + EPS)


def on_device(
    probe_vectors,
    source_vectors,
    content_vectors,
    probe_direction_matrix,
    probe_direction_source,
    content_direction,
    head_table_indices,
    reset_flags,
    projection_matrix,
    regression_goal,
):
    length = probe_vectors.shape[0]
    heads_here = head_table_indices.shape[0]
    head_width = probe_vectors.shape[1] // heads_here
    chain_len = length * lax.axis_size("seq")
    forgetting_exponent = log_gammas(head_table_indices, float(chain_len))
    fading_rate_exponent = segment_rate_exponents(reset_flags, forgetting_exponent)

    def to_heads(array):
        return array.astype(jnp.float32).reshape(length, heads_here, head_width)

    query_rows, key_rows, value_rows = (
        to_heads(probe_vectors),
        to_heads(source_vectors),
        to_heads(content_vectors),
    )
    query_tan, key_tan, value_tan = (
        to_heads(probe_direction_matrix),
        to_heads(probe_direction_source),
        to_heads(content_direction),
    )
    decay_all = jnp.exp(fading_rate_exponent[-1])
    state_own, state_tan = jax.jvp(
        lambda a, b: block_state(a, b, fading_rate_exponent),
        (key_rows, value_rows),
        (key_tan, value_tan),
    )
    state_in, state_in_tan = entering(jnp.stack([state_own, state_tan]), decay_all, False, 0)
    outputs, outputs_tan = jax.jvp(
        lambda a, b, c, d: block_out(a, b, c, d, fading_rate_exponent, PLAIN),
        (query_rows, key_rows, value_rows, state_in),
        (query_tan, key_tan, value_tan, state_in_tan),
    )
    normed, normed_tan = jax.jvp(group_norm, (outputs,), (outputs_tan,))
    normed_rows = normed.reshape(length, -1).astype(jnp.bfloat16)
    normed_rows_tan = normed_tan.reshape(length, -1).astype(jnp.bfloat16)
    both = middle(
        jnp.concatenate([normed_rows, normed_rows_tan]), projection_matrix, regression_goal
    )
    grad_norm = both[:length].reshape(length, heads_here, head_width)
    grad_norm_tan = both[length:].reshape(length, heads_here, head_width)

    def norm_back(point, cotan):
        return jax.vjp(group_norm, point)[1](cotan)[0]

    grad_out, grad_out_tan = jax.jvp(norm_back, (outputs, grad_norm), (outputs_tan, grad_norm_tan))

    def out_grads(a, b, c, d, g):
        return jax.vjp(
            lambda a2, b2, c2, d2: block_out(a2, b2, c2, d2, fading_rate_exponent, HIGHEST),
            a,
            b,
            c,
            d,
        )[1](g)

    primal_g, tangent_g = jax.jvp(
        out_grads,
        (query_rows, key_rows, value_rows, state_in, grad_out),
        (query_tan, key_tan, value_tan, state_in_tan, grad_out_tan),
    )
    returned = entering(jnp.stack([primal_g[3], tangent_g[3]]), decay_all, True, 1)

    def state_grads(b, c, g):
        return jax.vjp(lambda b2, c2: block_state(b2, c2, fading_rate_exponent), b, c)[1](g)

    extra_tan = jax.jvp(
        state_grads, (key_rows, value_rows, returned[0]), (key_tan, value_tan, returned[1])
    )[1]
    hess_q = tangent_g[0].reshape(length, -1).astype(jnp.bfloat16)
    hess_k = (tangent_g[1] + extra_tan[0]).reshape(length, -1).astype(jnp.bfloat16)
    hess_v = (tangent_g[2] + extra_tan[1]).reshape(length, -1).astype(jnp.bfloat16)
    return (hess_q, hess_k, hess_v)


def solution(mesh):
    in_specs = (
        P("seq", "head"),
        P("seq", "head"),
        P("seq", "head"),
        P("seq", "head"),
        P("seq", "head"),
        P("seq", "head"),
        P("head"),
        P("seq"),
        P("head", None),
        P("seq", None),
    )
    out_specs = (P("seq", "head"), P("seq", "head"), P("seq", "head"))
    return jax.shard_map(
        on_device, mesh=mesh, in_specs=in_specs, out_specs=out_specs, check_vma=False
    )
```
